256 devices in a mesh: parts: 4 (over y, x), space: 32 (over z), shot: 2 (over core).
Axes of the slice: x: 2, y: 2, z: 32, core: 2. Of those that a mesh axis runs over, the one named last changes fastest.
The devices are a block of a 4x8x32 slice.
Arguments:
- velocity: float32 [3072, 32, 384], P(('parts', 'space'), 'shot'), parts along dimension 0, may hold values from 1.5 to 4.5
- adjoint_now: float32 [16, 768, 32, 384], P(('parts', 'shot'), 'space'), parts along dimension 0, may hold values from -6 to 6
- adjoint_before: float32 [16, 768, 32, 384], P(('parts', 'shot'), 'space'), parts along dimension 0, may hold values from -6 to 6
- checkpoints: bfloat16 [16, 3, 768, 32, 384], P(('parts', 'shot'), None, 'space'), parts along dimension 0, may hold values from -6 to 6
- exponents: int32 [16, 3, 768, 32], P(('parts', 'shot'), None, 'space'), parts along dimension 0, may hold values from -2 to 2
- residuals: float32 [16, 3, 1024], P(('parts', 'shot')), parts along dimension 0, may hold values from -6 to 6
- receivers: int32 [16, 1024, 3], P(('parts', 'shot')), parts along dimension 0, may hold values from 0 to 767, as said below
- sources: int32 [16, 3], P(('parts', 'shot')), parts along dimension 0, may hold values from 0 to 767, as said below
Outputs:
- gradient: float32 [3072, 32, 384], P(('parts', 'space'), 'shot'), parts along dimension 0
- adjoint_next: float32 [16, 768, 32, 384], P(('parts', 'shot'), 'space'), parts along dimension 0
- adjoint_last: float32 [16, 768, 32, 384], P(('parts', 'shot'), 'space'), parts along dimension 0
The draws below stay inside these ranges and needn't reach their ends.
There are 4 independent parts, one for each index of `parts`. The reference program is written for one: setup_inputs(seed, part) draws one part's arguments, and reference() takes and returns one part's arrays. A program takes and returns all parts, laid end to end along the dimension named above; each array names one. Nothing has to cross between parts.
Inputs may be any that keep to these rules, and one draw needn't show every extreme that they name: `receivers`: each row holds a receiver's x, y and z cell index, each inside the grid. `sources`: each row holds the source's x, y and z cell index, each inside the grid.
All inputs are finite; a program needn't handle non-finite values.
Results may differ from the reference program's by a relative error of at most 0.0003.
Values sent between devices are 32-bit elements; how exact they have to be, the bound alone decides.
A program may use at most 128 MiB of HBM per device.

```python
import jax
import jax.numpy as jnp
from jax import lax

NY = 32
NZ = 384
NREC = 1024
STEPS = 3
MUTE = 6
NX = 768
SHOTS = 4


def cell_indices(key, count):
    keyx, keyy, keyz = jax.random.split(key, 3)
    xcells = jax.random.randint(keyx, count, 0, NX)
    ycells = jax.random.randint(keyy, count, 0, NY)
    zcells = jax.random.randint(keyz, count, 0, NZ)
    return jnp.stack((xcells, ycells, zcells), -1).astype(jnp.int32)


def draw_receivers(key, part):
    return cell_indices(jax.random.fold_in(key, 11), (SHOTS, NREC))


def draw_sources(key, part):
    return cell_indices(jax.random.fold_in(key, 23), (SHOTS,))


def plant(drawn, key, smallest, top_value):
    index_at = [jax.random.randint(jax.random.fold_in(key, axis), (), 0, length) for axis, length in enumerate(drawn.shape)]
    longest = drawn.shape.index(max(drawn.shape))
    next_to = index_at[:longest] + [(index_at[longest] + 1) % drawn.shape[longest]] + index_at[longest + 1:]
    return drawn.at[tuple(index_at)].set(smallest).at[tuple(next_to)].set(top_value)


def levels(stream_key, shape, pieces, least, high):
    gain, own = 1.0, jax.random.fold_in(stream_key, 6)
    for dim, parts in pieces:
        draws = jnp.exp(jax.random.uniform(jax.random.fold_in(own, dim), (parts,), jnp.float32, least / len(pieces), high / len(pieces)))
        gain = gain * jnp.repeat(draws, shape[dim] // parts).reshape([-1 if axis == dim else 1 for axis in range(len(shape))])
    return gain


def scatter_about(key, dims, scale, bound, cuts=(), kind=jnp.bfloat16):
    factor_of = levels(key, dims, cuts, -0.22, 0.18) if cuts else 1.0
    entries = jax.random.normal(key, dims, jnp.float32) * scale * factor_of
    return jnp.minimum(jnp.maximum(entries, -bound), bound).astype(kind)


def setup_inputs(seed: int = 0, part: int = 0) -> dict:
    key_of = jax.random.split(jax.random.key(seed), 9)
    part_splits = jax.random.split(jax.random.fold_in(key_of[8], part), 9)
    velocity = jnp.clip(1.5 + 3.0 * jax.random.uniform(part_splits[0], (NX, NY, NZ), jnp.float32) ** levels(part_splits[0], (NX, NY, NZ), ((0, 32), (1, 2)), -0.2, 0.2), 1.5, 4.5)
    adjoint_now = scatter_about(part_splits[1], (SHOTS, NX, NY, NZ), 1.0, 6.0, ((0, 2), (1, 32)), jnp.float32)
    adjoint_before = scatter_about(part_splits[2], (SHOTS, NX, NY, NZ), 1.0, 6.0, ((0, 2), (1, 32)), jnp.float32)
    checkpoints = scatter_about(part_splits[3], (SHOTS, STEPS, NX, NY, NZ), 1.0, 6.0, ((0, 2), (2, 32)))
    exponents = plant(jax.random.randint(part_splits[4], (SHOTS, STEPS, NX, NY), -2, 3), jax.random.fold_in(part_splits[4], 1), -2, 2).astype(jnp.int32)
    residuals = scatter_about(part_splits[5], (SHOTS, STEPS, NREC), 1.0, 6.0, ((0, 2),), jnp.float32)
    receivers = draw_receivers(jax.random.fold_in(jax.random.fold_in(key_of[8], part), 71), part)
    sources = draw_sources(jax.random.fold_in(jax.random.fold_in(key_of[8], part), 71), part)
    return {"velocity": velocity, "adjoint_now": adjoint_now, "adjoint_before": adjoint_before, "checkpoints": checkpoints, "exponents": exponents, "residuals": residuals, "receivers": receivers, "sources": sources}


coef_list = (-205.0 / 72.0, 8.0 / 5.0, -1.0 / 5.0, 8.0 / 315.0, -1.0 / 560.0)


def laplace(field):
    full = jnp.pad(field, 4)
    extent = field.shape

    def shifted(offx, offy, offz):
        return full[4 + offx:4 + offx + extent[0], 4 + offy:4 + offy + extent[1], 4 + offz:4 + offz + extent[2]]

    summed = 3.0 * coef_list[0] * field
    for offset in range(1, 5):
        summed = summed + coef_list[offset] * (shifted(offset, 0, 0) + shifted(-offset, 0, 0) + shifted(0, offset, 0) + shifted(0, -offset, 0) + shifted(0, 0, offset) + shifted(0, 0, -offset))
    return summed


def reference(velocity, adjoint_now, adjoint_before, checkpoints, exponents, residuals, receivers, sources):
    factor = (0.1 * velocity) ** 2
    xcoord = jnp.arange(NX, dtype=jnp.float32)
    ycoord = jnp.arange(NY, dtype=jnp.float32)
    zcoord = jnp.arange(NZ, dtype=jnp.float32)

    def one_shot(items):
        current, before, saved, powers, traces, places, anchor = items
        image = jnp.zeros_like(current)
        for step in range(STEPS):
            nxt = 2.0 * current - before + factor * laplace(current)
            nxt = nxt.at[places[:, 0], places[:, 1], places[:, 2]].add(traces[step])
            decoded = saved[step].astype(jnp.float32) * jnp.exp2(powers[step].astype(jnp.float32))[:, :, None]
            image = image + nxt * decoded
            before, current = current, nxt
        anchor_f = anchor.astype(jnp.float32)
        distance = (xcoord[:, None, None] - anchor_f[0]) ** 2 + (ycoord[None, :, None] - anchor_f[1]) ** 2 + (zcoord[None, None, :] - anchor_f[2]) ** 2
        mute = 1.0 - jnp.exp(-distance / (2.0 * MUTE * MUTE))
        return mute * image, current, before

    images, finals, priors = lax.map(one_shot, (adjoint_now, adjoint_before, checkpoints, exponents, residuals, receivers, sources))
    gradient = (2.0 / velocity) * jnp.sum(images, 0)
    return gradient, finals, priors
```

```python
import jax
import jax.numpy as jnp
from jax import lax
from jax.experimental import pallas as pl
from jax.experimental.pallas import tpu as pltpu
from jax.sharding import PartitionSpec as P

STEPS = 3
MUTE = 6
WIDE = 4
BLOCK = 8

coef_list = (-205.0 / 72.0, 8.0 / 5.0, -1.0 / 5.0, 8.0 / 315.0, -1.0 / 560.0)
UNIT = coef_list[1]
near = [c / UNIT for c in coef_list[1:]]
CENTRE = 3.0 * coef_list[0] / UNIT

F32 = jnp.float32
BF16 = jnp.bfloat16
MESH = pl.DeviceIdType.MESH
VMEM_LIMIT = 52 * 1024 * 1024


def band(gap):
    gap = jnp.abs(gap)
    out = jnp.zeros(gap.shape, F32)
    for k in range(WIDE):
        out = jnp.where(gap == k + 1, near[k], out)
    return out


def iota(shape, dim):
    return lax.broadcasted_iota(jnp.int32, shape, dim)


def kernel(
    v_hbm, now_hbm, before_hbm, ck_hbm, ex_hbm, res_hbm, rec_hbm, src_hbm,
    grad, nxt, last,
    before, now, mid, halo, speed, factor, ck, ex, res, rec, src,
    spread, hits, places, inj, lap, total, got, falls, along_y, along_z,
    in_sem, small_sem, v_send, v_recv, s_send, s_recv, g_send, g_recv,
):
    shots, cells, planes, depths = now.shape
    half = planes // 2
    rows = BLOCK * planes
    count = lax.axis_size("space")
    me = lax.axis_index("space")
    core = lax.axis_index("shot")
    has_left = me > 0
    has_right = me < count - 1
    mine = pl.multiple_of(core * half, half)
    theirs = pl.multiple_of((1 - core) * half, half)
    inner = cells - 2 * WIDE
    fields = (before, now, mid, last, nxt)

    def local(src_ref, dst_ref, sem):
        copy = pltpu.make_async_copy(src_ref, dst_ref, sem)
        copy.start()
        return copy

    small = [
        local(rec_hbm, rec, small_sem.at[0]),
        local(res_hbm, res, small_sem.at[1]),
        local(ex_hbm, ex, small_sem.at[2]),
        local(src_hbm, src, small_sem.at[3]),
        local(v_hbm, speed.at[:, pl.ds(mine, half)], small_sem.at[4]),
    ]
    loads = []
    for s in range(shots):
        loads.append(
            [
                local(now_hbm.at[s], now.at[s], in_sem.at[s, 0]),
                local(before_hbm.at[s], before.at[s], in_sem.at[s, 1]),
                local(ck_hbm.at[s], ck.at[s], in_sem.at[s, 2]),
            ]
        )

    barrier = pltpu.get_barrier_semaphore()
    pl.semaphore_signal(barrier, inc=1, device_id={"shot": 1 - core}, device_id_type=MESH)

    @pl.when(has_left)
    def _():
        pl.semaphore_signal(barrier, inc=1, device_id={"space": me - 1}, device_id_type=MESH)

    @pl.when(has_right)
    def _():
        pl.semaphore_signal(barrier, inc=1, device_id={"space": me + 1}, device_id_type=MESH)

    pl.semaphore_wait(barrier, 1 + has_left.astype(jnp.int32) + has_right.astype(jnp.int32))

    def sending(s, t, side):
        source = now_hbm if t == 0 else fields[t + 1]
        first = cells - WIDE if side == 0 else 0
        return pltpu.make_async_remote_copy(
            src_ref=source.at[s, pl.ds(first, WIDE)],
            dst_ref=halo.at[t, s, side],
            send_sem=s_send.at[t, s, side],
            recv_sem=s_recv.at[t, s, side],
            device_id={"space": me + 1 if side == 0 else me - 1},
            device_id_type=MESH,
        )

    sides = ((0, has_right, has_left), (1, has_left, has_right))

    def send(s, t):
        for side, out, _ in sides:

            @pl.when(out)
            def _():
                sending(s, t, side).start()

    def arrived(s, t):
        for side, _, came in sides:

            @pl.when(came)
            def _():
                sending(s, t, side).wait_recv()

    for s in range(shots):
        send(s, 0)
    v_copy = pltpu.make_async_remote_copy(
        src_ref=v_hbm,
        dst_ref=speed.at[:, pl.ds(mine, half)],
        send_sem=v_send,
        recv_sem=v_recv,
        device_id={"shot": 1 - core},
        device_id_type=MESH,
    )
    v_copy.start()

    for side, _, came in sides:

        @pl.when(jnp.logical_not(came))
        def _():
            for t in range(STEPS):
                for s in range(shots):
                    halo[t, s, side] = jnp.zeros((WIDE, planes, depths), F32)

    gap = iota((depths, depths), 0) - iota((depths, depths), 1)
    bands = band(gap).astype(BF16)
    along_z[:depths] = bands
    along_z[depths:] = bands
    at_row = iota((rows, rows), 0)
    at_col = iota((rows, rows), 1)
    log_planes = planes.bit_length() - 1
    same = (at_row >> log_planes) == (at_col >> log_planes)
    along_y[...] = jnp.where(same, band(at_row - at_col), 0.0).astype(BF16)

    for copy in small[:4]:
        copy.wait()

    receivers = rec.shape[2]
    for s in range(shots):
        local_x = rec[0, pl.ds(s, 1)] - me * cells
        inside = (local_x >= 0) & (local_x < cells)
        row = jnp.where(inside, local_x * planes + rec[1, pl.ds(s, 1)], -1)
        hit = iota((cells * planes, receivers), 0) == row
        hits[s] = jnp.where(hit, 1.0, 0.0).astype(BF16)

    def inject(s, steps):
        depth_hit = iota((depths, receivers), 0) == rec[2, pl.ds(s, 1)]
        for i, t in enumerate(steps):
            value = res[t, pl.ds(s, 1)]
            high = value.astype(BF16).astype(F32)
            low = value - high
            to = pl.ds(i * depths, depths)
            places[to, :receivers] = jnp.where(depth_hit, high, 0.0).astype(BF16)
            places[to, receivers:] = jnp.where(depth_hit, low, 0.0).astype(BF16)
        onehot = hits[s]
        added = lax.dot_general(
            jnp.concatenate([onehot, onehot], axis=1),
            places[: len(steps) * depths],
            (((1,), (1,)), ((), ())),
            preferred_element_type=F32,
        )
        for i, t in enumerate(steps):
            inj[t, s] = added[:, i * depths : (i + 1) * depths].reshape(cells, planes, depths)

    for s in range(shots):
        inject(s, (0,))

    eye = jnp.where(iota((planes, planes), 0) == iota((planes, planes), 1), 1.0, 0.0)
    ones = jnp.ones((planes, 128), BF16)
    for s in range(shots):
        for t in range(STEPS):
            scale = jnp.exp2(ex[s, t].astype(F32))
            diag = scale[:, None, :] * eye[None]
            diag = diag.reshape(cells * planes, planes).astype(BF16)
            wide = jnp.dot(diag, ones, preferred_element_type=F32)
            spread[t, s] = wide.reshape(cells, planes, 128)

    small[4].wait()
    v_copy.wait()
    v = speed[...]
    factor[...] = (0.01 * UNIT) * v * v
    total[...] = jnp.zeros_like(total)

    for s in range(shots):
        dy = (iota((planes, depths), 0) - src[s, 1]).astype(F32)
        dz = (iota((planes, depths), 1) - src[s, 2]).astype(F32)
        falls[s] = jnp.exp((dy * dy + dz * dz) * (-1.0 / (2.0 * MUTE * MUTE)))

    def split(c):
        high = c.astype(BF16)
        return high, (c - high.astype(F32)).astype(BF16)

    def crossed(c):
        high, low = split(c)
        by_z = jnp.dot(
            jnp.concatenate([high, low], axis=1), along_z[...], preferred_element_type=F32
        )
        by_y = jnp.dot(along_y[...], high, preferred_element_type=F32) + jnp.dot(
            along_y[...], low, preferred_element_type=F32
        )
        return by_z + by_y

    def plane(s, t, x, read, yz):
        c = read(0)
        acc = yz + CENTRE * c
        for k in range(WIDE):
            pair = read(k + 1) + read(-k - 1)
            acc = acc + (pair if k == 0 else near[k] * pair)
        new = (c + c - fields[t][s, x]) + factor[x] * acc + inj[t, s, x]
        fields[t + 2][s, x] = new
        scale = spread[t, s, x]
        scale = jnp.concatenate([scale] * (depths // 128), axis=1)
        dx = (me * cells + x - src[s, 0]).astype(F32)
        fall = jnp.exp(jnp.full((planes, 128), dx * dx * (-1.0 / (2.0 * MUTE * MUTE)), F32))
        fall = jnp.concatenate([fall] * (depths // 128), axis=1)
        mute = 1.0 - fall * falls[s]
        total[x] = total[x] + mute * (new * (ck[s, t, x].astype(F32) * scale))

    def interior(s, t):
        p = fields[t + 1]

        def block(b, _):
            x0 = WIDE + b * BLOCK
            lap[...] = crossed(p[s, pl.ds(x0, BLOCK)].reshape(rows, depths)).reshape(
                BLOCK, planes, depths
            )

            def one(i, _):
                x = x0 + i
                plane(s, t, x, lambda k: p[s, x + k], lap[i])
                return 0

            lax.fori_loop(0, BLOCK, one, 0)
            return 0

        lax.fori_loop(0, inner // BLOCK, block, 0)

    def boundary(s, t):
        p = fields[t + 1]

        def at(x):
            if x < 0:
                return halo[t, s, 0, x + WIDE]
            if x >= cells:
                return halo[t, s, 1, x - cells]
            return p[s, x]

        edges = jnp.concatenate([p[s, :WIDE], p[s, cells - WIDE :]], axis=0)
        lap[...] = crossed(edges.reshape(rows, depths)).reshape(BLOCK, planes, depths)
        for i in range(BLOCK):
            x = i if i < WIDE else cells - BLOCK + i
            plane(s, t, x, lambda k: at(x + k), lap[i])

    def loaded(s):
        for copy in loads[s]:
            copy.wait()

    pieces = ((WIDE, inner), (0, WIDE), (cells - WIDE, WIDE))

    def give(piece):
        first, size = pieces[piece]
        return pltpu.make_async_remote_copy(
            src_ref=total.at[pl.ds(first, size), pl.ds(theirs, half)],
            dst_ref=got.at[pl.ds(first, size)],
            send_sem=g_send.at[piece],
            recv_sem=g_recv.at[piece],
            device_id={"shot": 1 - core},
            device_id_type=MESH,
        )

    def finish(piece):
        first, size = pieces[piece]
        at = pl.ds(first, size)
        ours = total[at, pl.ds(mine, half)] + got[at]
        grad[at] = (2.0 / speed[at, pl.ds(mine, half)]) * ours

    loaded(0)
    interior(0, 0)
    loaded(1)
    order = [(s, t) for t in range(STEPS) for s in range(shots)]
    for p, (s, t) in enumerate(order):
        arrived(s, t)
        boundary(s, t)
        if t < STEPS - 1:
            send(s, t + 1)
        if p + 1 < len(order):
            interior(*order[p + 1])
        if t == 0:
            inject(s, tuple(range(1, STEPS)))
        if p + 2 == len(order):
            give(0).start()

    give(1).start()
    give(2).start()
    for piece in range(3):
        give(piece).wait_recv()
        finish(piece)
    for piece in range(3):
        give(piece).wait_send()
    for s, t in order:
        for side, out, _ in sides:

            @pl.when(out)
            def _():
                sending(s, t, side).wait_send()


def body(
    velocity, adjoint_now, adjoint_before, checkpoints, exponents, residuals, receivers, sources
):
    shots, cells, planes, depths = adjoint_now.shape
    count = receivers.shape[1]
    half = planes // 2
    rows = BLOCK * planes
    hbm = pl.BlockSpec(memory_space=pltpu.HBM)
    vmem = pl.BlockSpec(memory_space=pltpu.VMEM)
    dma = pltpu.SemaphoreType.DMA
    sent = (STEPS, shots, 2)
    return pl.pallas_call(
        kernel,
        out_shape=(
            pltpu.VMEM((cells, half, depths), F32),
            pltpu.VMEM((shots, cells, planes, depths), F32),
            pltpu.VMEM((shots, cells, planes, depths), F32),
        ),
        in_specs=[hbm] * 8,
        out_specs=(vmem, vmem, vmem),
        scratch_shapes=[
            pltpu.VMEM((shots, cells, planes, depths), F32),
            pltpu.VMEM((shots, cells, planes, depths), F32),
            pltpu.VMEM((shots, cells, planes, depths), F32),
            pltpu.VMEM((*sent, WIDE, planes, depths), F32),
            pltpu.VMEM((cells, planes, depths), F32),
            pltpu.VMEM((cells, planes, depths), F32),
            pltpu.VMEM((shots, STEPS, cells, planes, depths), BF16),
            pltpu.VMEM((shots, STEPS, cells, planes), jnp.int32),
            pltpu.VMEM((STEPS, shots, count), F32),
            pltpu.VMEM((3, shots, count), jnp.int32),
            pltpu.SMEM((shots, 3), jnp.int32),
            pltpu.VMEM((STEPS, shots, cells, planes, 128), F32),
            pltpu.VMEM((shots, cells * planes, count), BF16),
            pltpu.VMEM(((STEPS - 1) * depths, 2 * count), BF16),
            pltpu.VMEM((STEPS, shots, cells, planes, depths), F32),
            pltpu.VMEM((BLOCK, planes, depths), F32),
            pltpu.VMEM((cells, planes, depths), F32),
            pltpu.VMEM((cells, half, depths), F32),
            pltpu.VMEM((shots, planes, depths), F32),
            pltpu.VMEM((rows, rows), BF16),
            pltpu.VMEM((2 * depths, depths), BF16),
            dma((shots, 3)),
            dma((5,)),
            dma(()),
            dma(()),
            dma(sent),
            dma(sent),
            dma((3,)),
            dma((3,)),
        ],
        compiler_params=pltpu.CompilerParams(
            collective_id=0, has_side_effects=True, vmem_limit_bytes=VMEM_LIMIT
        ),
    )(
        velocity,
        adjoint_now,
        adjoint_before,
        checkpoints,
        exponents,
        jnp.transpose(residuals, (1, 0, 2)),
        jnp.transpose(receivers, (2, 0, 1)),
        sources,
    )


def solution(mesh):
    placed = (
        P(("parts", "space"), "shot", None),
        P(("parts", "shot"), "space", None, None),
        P(("parts", "shot"), "space", None, None),
        P(("parts", "shot"), None, "space", None, None),
        P(("parts", "shot"), None, "space", None),
        P(("parts", "shot"), None, None),
        P(("parts", "shot"), None, None),
        P(("parts", "shot"), None),
    )
    return jax.shard_map(
        body,
        mesh=mesh,
        in_specs=placed,
        out_specs=(
            P(("parts", "space"), "shot", None),
            P(("parts", "shot"), "space", None, None),
            P(("parts", "shot"), "space", None, None),
        ),
        check_vma=False,
    )
```

```python
import jax
import jax.numpy as jnp
from jax import lax
from jax.experimental import pallas as pl
from jax.experimental.pallas import tpu as pltpu
from jax.sharding import PartitionSpec as P

STEPS = 3
MUTE = 6
WIDE = 4
BLOCK = 8

coef_list = (-205.0 / 72.0, 8.0 / 5.0, -1.0 / 5.0, 8.0 / 315.0, -1.0 / 560.0)
UNIT = coef_list[1]
near = [c / UNIT for c in coef_list[1:]]
CENTRE = 3.0 * coef_list[0] / UNIT

F32 = jnp.float32
BF16 = jnp.bfloat16
MESH = pl.DeviceIdType.MESH
LANES = 128
VMEM_LIMIT = 54 * 1024 * 1024


def band(gap):
    gap = jnp.abs(gap)
    out = jnp.zeros(gap.shape, F32)
    for k in range(WIDE):
        out = jnp.where(gap == k + 1, near[k], out)
    return out


def iota(shape, dim):
    return lax.broadcasted_iota(jnp.int32, shape, dim)


def kernel(
    v_hbm, now_hbm, before_hbm, ck_hbm, ex_hbm, res_hbm, rec_hbm, src_hbm,
    grad, nxt, last,
    before, now, mid, halo, speed, factor, ck, ex, res, rec, src,
    gain, mute, spread, hits, places, inj, lap, parts, total, got, along_y, along_z, along_z_end,
    in_sem, small_sem, v_send, v_recv, s_send, s_recv, g_send, g_recv,
):
    shots, cells, planes, depths = now.shape
    half = planes // 2
    rows = BLOCK * planes
    count = lax.axis_size("space")
    me = lax.axis_index("space")
    core = lax.axis_index("shot")
    has_left = me > 0
    has_right = me < count - 1
    mine = pl.multiple_of(core * half, half)
    theirs = pl.multiple_of((1 - core) * half, half)
    inner = cells - 2 * WIDE
    fields = (before, now, mid, last, nxt)

    def local(src_ref, dst_ref, sem):
        copy = pltpu.make_async_copy(src_ref, dst_ref, sem)
        copy.start()
        return copy

    small = [
        local(rec_hbm, rec, small_sem.at[0]),
        local(res_hbm, res, small_sem.at[1]),
        local(ex_hbm, ex, small_sem.at[2]),
        local(src_hbm, src, small_sem.at[3]),
        local(v_hbm, speed.at[:, pl.ds(mine, half)], small_sem.at[4]),
    ]
    loads = []
    for s in range(shots):
        loads.append(
            [
                local(now_hbm.at[s], now.at[s], in_sem.at[s, 0]),
                local(before_hbm.at[s], before.at[s], in_sem.at[s, 1]),
                local(ck_hbm.at[s], ck.at[s], in_sem.at[s, 2]),
            ]
        )

    barrier = pltpu.get_barrier_semaphore()
    pl.semaphore_signal(barrier, inc=1, device_id={"shot": 1 - core}, device_id_type=MESH)

    @pl.when(has_left)
    def _():
        pl.semaphore_signal(barrier, inc=1, device_id={"space": me - 1}, device_id_type=MESH)

    @pl.when(has_right)
    def _():
        pl.semaphore_signal(barrier, inc=1, device_id={"space": me + 1}, device_id_type=MESH)

    pl.semaphore_wait(barrier, 1 + has_left.astype(jnp.int32) + has_right.astype(jnp.int32))

    def sending(s, t, side):
        source = now_hbm if t == 0 else fields[t + 1]
        first = cells - WIDE if side == 0 else 0
        return pltpu.make_async_remote_copy(
            src_ref=source.at[s, pl.ds(first, WIDE)],
            dst_ref=halo.at[t, s, side],
            send_sem=s_send.at[t, s, side],
            recv_sem=s_recv.at[t, s, side],
            device_id={"space": me + 1 if side == 0 else me - 1},
            device_id_type=MESH,
        )

    sides = ((0, has_right, has_left), (1, has_left, has_right))

    def send(s, t):
        for side, out, _ in sides:

            @pl.when(out)
            def _():
                sending(s, t, side).start()

    def arrived(s, t):
        for side, _, came in sides:

            @pl.when(came)
            def _():
                sending(s, t, side).wait_recv()

    for s in range(shots):
        send(s, 0)
    v_copy = pltpu.make_async_remote_copy(
        src_ref=v_hbm,
        dst_ref=speed.at[:, pl.ds(mine, half)],
        send_sem=v_send,
        recv_sem=v_recv,
        device_id={"shot": 1 - core},
        device_id_type=MESH,
    )
    v_copy.start()

    for side, _, came in sides:

        @pl.when(jnp.logical_not(came))
        def _():
            for t in range(STEPS):
                for s in range(shots):
                    halo[t, s, side] = jnp.zeros((WIDE, planes, depths), F32)

    gap = iota((depths, depths), 0) - iota((depths, depths), 1)
    bands = band(gap).astype(BF16)
    first = 2 * LANES
    along_z[:depths] = bands[:, :first]
    along_z[depths:] = bands[:, :first]
    along_z_end[: depths - LANES] = bands[LANES:, first:]
    along_z_end[depths - LANES :] = bands[LANES:, first:]
    at_row = iota((rows, rows), 0)
    at_col = iota((rows, rows), 1)
    log_planes = planes.bit_length() - 1
    same = (at_row >> log_planes) == (at_col >> log_planes)
    within = jnp.where(same, band(at_row - at_col), 0.0).astype(BF16)
    along_y[:, :rows] = within
    along_y[:, rows:] = within

    for copy in small[:4]:
        copy.wait()

    receivers = rec.shape[2]
    for s in range(shots):
        local_x = rec[0, pl.ds(s, 1)] - me * cells
        inside = (local_x >= 0) & (local_x < cells)
        row = jnp.where(inside, local_x * planes + rec[1, pl.ds(s, 1)], -1)
        hit = iota((cells * planes, receivers), 0) == row
        hits[s] = jnp.where(hit, 1.0, 0.0).astype(BF16)

    def inject(s, steps):
        depth_hit = iota((depths, receivers), 0) == rec[2, pl.ds(s, 1)]
        for i, t in enumerate(steps):
            value = res[t, pl.ds(s, 1)]
            high = value.astype(BF16).astype(F32)
            low = value - high
            to = pl.ds(i * depths, depths)
            places[to, :receivers] = jnp.where(depth_hit, high, 0.0).astype(BF16)
            places[to, receivers:] = jnp.where(depth_hit, low, 0.0).astype(BF16)
        onehot = hits[s]
        added = lax.dot_general(
            jnp.concatenate([onehot, onehot], axis=1),
            places[: len(steps) * depths],
            (((1,), (1,)), ((), ())),
            preferred_element_type=F32,
        )
        for i, t in enumerate(steps):
            inj[t, s] = added[:, i * depths : (i + 1) * depths].reshape(cells, planes, depths)

    inject(0, (0,))

    eye = jnp.where(iota((planes, planes), 0) == iota((planes, planes), 1), 1.0, 0.0)
    ones = jnp.ones((planes, LANES), BF16)
    for s in range(shots):
        for t in range(STEPS):
            scale = jnp.exp2(ex[s, t].astype(F32))
            diag = scale[:, None, :] * eye[None]
            diag = diag.reshape(cells * planes, planes).astype(BF16)
            wide = jnp.dot(diag, ones, preferred_element_type=F32)
            spread[t, s] = wide.reshape(cells, planes, LANES)

    small[4].wait()
    v_copy.wait()
    v = speed[...]
    f = (0.01 * UNIT) * v * v
    factor[...] = f
    gain[...] = 2.0 + CENTRE * f
    total[...] = jnp.zeros_like(total)

    fade = -1.0 / (2.0 * MUTE * MUTE)
    for s in range(shots):
        dy = (iota((planes, depths), 0) - src[s, 1]).astype(F32)
        dz = (iota((planes, depths), 1) - src[s, 2]).astype(F32)
        fall = jnp.exp((dy * dy + dz * dz) * fade)
        dx = (iota((cells, planes, LANES), 0) + (me * cells - src[s, 0])).astype(F32)
        fall_x = jnp.exp(dx * dx * fade)
        for z in range(0, depths, LANES):
            mute[s, :, :, z : z + LANES] = 1.0 - fall_x * fall[None, :, z : z + LANES]

    edge = tuple(range(WIDE)) + tuple(range(cells - WIDE, cells))
    spans = tuple(
        tuple(range(x, x + BLOCK)) for x in range(WIDE, cells - WIDE, BLOCK)
    ) + (edge,)
    work = [
        (s, t, span, span is edge) for t in range(STEPS) for s in range(shots) for span in spans
    ]

    def crossed(k):
        s, t, span, _ = work[k]
        slot = k % 2
        for i, x in enumerate(span):
            c = fields[t + 1][s, x]
            high = c.astype(BF16)
            at = slice(i * planes, (i + 1) * planes)
            parts[slot, 0, at] = high
            parts[slot, 1, at] = (c - high.astype(F32)).astype(BF16)
        high, low = parts[slot, 0], parts[slot, 1]
        by_y = jnp.dot(
            along_y[...], jnp.concatenate([high, low], axis=0), preferred_element_type=F32
        )
        by_z = jnp.dot(
            jnp.concatenate([high, low], axis=1), along_z[...], preferred_element_type=F32
        )
        lap[slot, :, :first] = by_y[:, :first] + by_z
        by_z = jnp.dot(
            jnp.concatenate([high[:, LANES:], low[:, LANES:]], axis=1),
            along_z_end[...],
            preferred_element_type=F32,
        )
        lap[slot, :, first:] = by_y[:, first:] + by_z

    def stepped(k):
        s, t, span, _ = work[k]
        p = fields[t + 1]

        def at(x, z):
            if x < 0:
                return halo[t, s, 0, x + WIDE, :, z]
            if x >= cells:
                return halo[t, s, 1, x - cells, :, z]
            return p[s, x, :, z]

        for i, x in enumerate(span):
            scale = spread[t, s, x]
            for z0 in range(0, depths, LANES):
                z = slice(z0, z0 + LANES)
                acc = lap[k % 2, i * planes : (i + 1) * planes, z]
                for d in range(WIDE):
                    pair = at(x + d + 1, z) + at(x - d - 1, z)
                    acc = acc + (pair if d == 0 else near[d] * pair)
                new = (gain[x, :, z] * at(x, z) - fields[t][s, x, :, z]) + (
                    factor[x, :, z] * acc + inj[t, s, x, :, z]
                )
                fields[t + 2][s, x, :, z] = new
                seen = mute[s, x, :, z] * (ck[s, t, x, :, z].astype(F32) * scale)
                total[x, :, z] = total[x, :, z] + new * seen

    def loaded(s):
        for copy in loads[s]:
            copy.wait()

    pieces = ((WIDE, inner), (0, WIDE), (cells - WIDE, WIDE))

    def give(piece):
        first, size = pieces[piece]
        return pltpu.make_async_remote_copy(
            src_ref=total.at[pl.ds(first, size), pl.ds(theirs, half)],
            dst_ref=got.at[pl.ds(first, size)],
            send_sem=g_send.at[piece],
            recv_sem=g_recv.at[piece],
            device_id={"shot": 1 - core},
            device_id_type=MESH,
        )

    def finish(piece):
        first, size = pieces[piece]
        at = pl.ds(first, size)
        ours = total[at, pl.ds(mine, half)] + got[at]
        grad[at] = (2.0 / speed[at, pl.ds(mine, half)]) * ours

    loaded(0)
    crossed(0)
    for k, (s, t, _, at_edge) in enumerate(work):
        if at_edge:
            if k < len(spans):
                loaded(1)
                inject(1, (0,))
            arrived(s, t)
        stepped(k)
        if k + 1 < len(work):
            crossed(k + 1)
        if at_edge and t < STEPS - 1:
            send(s, t + 1)
        if at_edge and k + 1 >= shots * len(spans) and k + 1 < 2 * shots * len(spans):
            inject((k + 1) // len(spans) - shots, tuple(range(1, STEPS)))
        if k + 2 == len(work):
            give(0).start()

    give(1).start()
    give(2).start()
    for piece in range(3):
        give(piece).wait_recv()
        finish(piece)
    for piece in range(3):
        give(piece).wait_send()
    for s, t in ((s, t) for t in range(STEPS) for s in range(shots)):
        for side, out, _ in sides:

            @pl.when(out)
            def _():
                sending(s, t, side).wait_send()


def written(*refs):
    inputs, outputs, sems = refs[:3], refs[3:6], refs[6]
    copies = []
    for i, (src, dst) in enumerate(zip(inputs, outputs)):
        size = src.shape[0] // 2
        for piece in range(2):
            at = pl.ds(piece * size, size)
            copy = pltpu.make_async_copy(src.at[at], dst.at[at], sems.at[i, piece])
            copy.start()
            copies.append(copy)
    for copy in copies:
        copy.wait()


def body(
    velocity, adjoint_now, adjoint_before, checkpoints, exponents, residuals, receivers, sources
):
    shots, cells, planes, depths = adjoint_now.shape
    count = receivers.shape[1]
    half = planes // 2
    rows = BLOCK * planes
    hbm = pl.BlockSpec(memory_space=pltpu.HBM)
    vmem = pl.BlockSpec(memory_space=pltpu.VMEM)
    dma = pltpu.SemaphoreType.DMA
    sent = (STEPS, shots, 2)
    results = pl.pallas_call(
        kernel,
        out_shape=(
            pltpu.VMEM((cells, half, depths), F32),
            pltpu.VMEM((shots, cells, planes, depths), F32),
            pltpu.VMEM((shots, cells, planes, depths), F32),
        ),
        in_specs=[hbm] * 8,
        out_specs=(vmem, vmem, vmem),
        scratch_shapes=[
            pltpu.VMEM((shots, cells, planes, depths), F32),
            pltpu.VMEM((shots, cells, planes, depths), F32),
            pltpu.VMEM((shots, cells, planes, depths), F32),
            pltpu.VMEM((*sent, WIDE, planes, depths), F32),
            pltpu.VMEM((cells, planes, depths), F32),
            pltpu.VMEM((cells, planes, depths), F32),
            pltpu.VMEM((shots, STEPS, cells, planes, depths), BF16),
            pltpu.VMEM((shots, STEPS, cells, planes), jnp.int32),
            pltpu.VMEM((STEPS, shots, count), F32),
            pltpu.VMEM((3, shots, count), jnp.int32),
            pltpu.SMEM((shots, 3), jnp.int32),
            pltpu.VMEM((cells, planes, depths), F32),
            pltpu.VMEM((shots, cells, planes, depths), F32),
            pltpu.VMEM((STEPS, shots, cells, planes, LANES), F32),
            pltpu.VMEM((shots, cells * planes, count), BF16),
            pltpu.VMEM(((STEPS - 1) * depths, 2 * count), BF16),
            pltpu.VMEM((STEPS, shots, cells, planes, depths), F32),
            pltpu.VMEM((2, rows, depths), F32),
            pltpu.VMEM((2, 2, rows, depths), BF16),
            pltpu.VMEM((cells, planes, depths), F32),
            pltpu.VMEM((cells, half, depths), F32),
            pltpu.VMEM((rows, 2 * rows), BF16),
            pltpu.VMEM((2 * depths, 2 * LANES), BF16),
            pltpu.VMEM((2 * (depths - LANES), depths - 2 * LANES), BF16),
            dma((shots, 3)),
            dma((5,)),
            dma(()),
            dma(()),
            dma(sent),
            dma(sent),
            dma((3,)),
            dma((3,)),
        ],
        compiler_params=pltpu.CompilerParams(
            collective_id=0, has_side_effects=True, vmem_limit_bytes=VMEM_LIMIT
        ),
    )(
        velocity,
        adjoint_now,
        adjoint_before,
        checkpoints,
        exponents,
        jnp.transpose(residuals, (1, 0, 2)),
        jnp.transpose(receivers, (2, 0, 1)),
        sources,
    )
    return pl.pallas_call(
        written,
        out_shape=tuple(jax.ShapeDtypeStruct(r.shape, r.dtype) for r in results),
        in_specs=[vmem] * 3,
        out_specs=(hbm,) * 3,
        scratch_shapes=[dma((3, 2))],
        compiler_params=pltpu.CompilerParams(vmem_limit_bytes=1024 * 1024),
    )(*(pltpu.with_memory_space_constraint(r, pltpu.VMEM) for r in results))


def solution(mesh):
    placed = (
        P(("parts", "space"), "shot", None),
        P(("parts", "shot"), "space", None, None),
        P(("parts", "shot"), "space", None, None),
        P(("parts", "shot"), None, "space", None, None),
        P(("parts", "shot"), None, "space", None),
        P(("parts", "shot"), None, None),
        P(("parts", "shot"), None, None),
        P(("parts", "shot"), None),
    )
    return jax.shard_map(
        body,
        mesh=mesh,
        in_specs=placed,
        out_specs=(
            P(("parts", "space"), "shot", None),
            P(("parts", "shot"), "space", None, None),
            P(("parts", "shot"), "space", None, None),
        ),
        check_vma=False,
    )
```
